32 devices in a mesh: section: 4 (over y, x), sc: 8 (over z, core).
Axes of the slice: x: 2, y: 2, z: 4, core: 2. Of those that a mesh axis runs over, the one named last changes fastest.
Arguments:
- observed_vector: float32 [1024, 14, 128], P('sc'), may hold values from -6 to 6
- propagation_matrix: float32 [1024, 8, 4, 128], P('sc', 'section'), may hold values from -0.5 to 0.5
- noise_var: float32 [1024], P('sc'), may hold values from 0.005 to 2.5, as said below
- sliced_constellation: int32 [1024, 14, 32], P('sc', None, 'section'), may hold values from 0 to 15
- detection_sequence: int32 [8], replicated, may hold values from 0 to 7, as said below
Outputs:
- estimates: float32 [1024, 14, 64], P('sc', None, 'section')
The draws below stay inside these ranges and needn't reach their ends.
Inputs may be any that keep to these rules, and one draw needn't show every extreme that they name: `noise_var`: positive variances. `detection_sequence`: a permutation taken in blocks of 2 positions: each block of positions holds the 2 group ids 2 * m to 2 * m + 1 of one m, in a rotated order; the first block of positions takes m = 2, the second m = 0.
All inputs are finite; a program needn't handle non-finite values.
Results may differ from the reference program's by a relative error of at most 0.0001.
Values sent between devices are 32-bit elements; how exact they have to be, the bound alone decides.
A program may use at most 64 MiB of HBM per device.

```python
import jax
import jax.numpy as jnp
from jax import lax

SENSOR_ELEMENTS = 64
TERMINAL_COUNT = 4
OFDM_TIME_SLOTS = 14
GRP_DEV = 2
TONE_COUNT = 1024
CLUSTER_COUNT = 8


def draw_noise_var(key, part):
    sequence_index = jnp.arange(TONE_COUNT, dtype=jnp.float32) / TONE_COUNT
    base = 0.01 * jnp.exp(sequence_index * 4.605170186)
    multiplier = jnp.exp(jax.random.uniform(key, (TONE_COUNT,), jnp.float32, -0.35, 0.35))
    return base * multiplier


def force_entry(order, where_slot, wanted):
    present = order[where_slot]
    order = jnp.where(order == wanted, present, order)
    return order.at[where_slot].set(wanted)


def draw_detection_sequence(key, part):
    block_count = CLUSTER_COUNT // GRP_DEV
    order = jax.random.permutation(jax.random.fold_in(key, 11), block_count).astype(jnp.int32)
    order = force_entry(order, 0, block_count // 2)
    order = force_entry(order, 1, 0)
    offsets = jax.random.randint(jax.random.fold_in(key, 12), (block_count,), 0, GRP_DEV, dtype=jnp.int32)
    within = jnp.arange(GRP_DEV, dtype=jnp.int32)
    sequence = GRP_DEV * order[:, None] + (within[None, :] + offsets[:, None]) % GRP_DEV
    return sequence.reshape(-1).astype(jnp.int32)


def set_ends(values, rng, smallest, largest):
    longest = values.shape.index(max(values.shape))
    spots = []
    for shift in (0, 1):
        where = [jax.random.randint(jax.random.fold_in(rng, axis), (), 0, length) for axis, length in enumerate(values.shape)]
        where[longest] = (where[longest] + shift) % values.shape[longest]
        spots.append(tuple(where))
    return values.at[spots[0]].set(smallest).at[spots[1]].set(largest)


def shard_levels(rng, dims, cuts, least, largest):
    def one(axis_at, parts):
        steps = jax.random.uniform(jax.random.fold_in(jax.random.fold_in(rng, 6), axis_at), (parts,), jnp.float32, least / len(cuts), largest / len(cuts))
        return jnp.repeat(jnp.exp(steps), dims[axis_at] // parts).reshape((-1,) + (1,) * (len(dims) - axis_at - 1))

    factor_of = one(*cuts[0])
    for cut in cuts[1:]:
        factor_of = factor_of * one(*cut)
    return factor_of


def centred(rng, dims, scale, limit, shards=(), kind=jnp.bfloat16):
    drawn = scale * jax.random.normal(rng, dims, jnp.float32)
    if shards:
        drawn = drawn * shard_levels(rng, dims, shards, -0.22, 0.18)
    return jnp.clip(drawn, -limit, limit).astype(kind)


def setup_inputs(seed: int = 0) -> dict:
    arg_keys = jax.random.split(jax.random.key(seed), 6)
    observed_vector = centred(arg_keys[0], (TONE_COUNT, OFDM_TIME_SLOTS, 2 * SENSOR_ELEMENTS), 1.0, 6.0, ((0, 8),), jnp.float32)
    propagation_matrix = centred(arg_keys[1], (TONE_COUNT, CLUSTER_COUNT, TERMINAL_COUNT, 2 * SENSOR_ELEMENTS), (2 * SENSOR_ELEMENTS) ** -0.5, 0.5, ((0, 8), (1, 4)), jnp.float32)
    noise_var = draw_noise_var(jax.random.fold_in(arg_keys[5], 71), 0)
    sliced_constellation = set_ends(jax.random.randint(arg_keys[3], (TONE_COUNT, OFDM_TIME_SLOTS, CLUSTER_COUNT * TERMINAL_COUNT), 0, 16), jax.random.fold_in(arg_keys[3], 1), 0, 15).astype(jnp.int32)
    detection_sequence = draw_detection_sequence(jax.random.fold_in(arg_keys[5], 71), 0)
    return {"observed_vector": observed_vector, "propagation_matrix": propagation_matrix, "noise_var": noise_var, "sliced_constellation": sliced_constellation, "detection_sequence": detection_sequence}


ROOT_TEN = 3.1622776601683795

def rotate(vectors):
    half = vectors.shape[-1] // 2
    return jnp.concatenate([-vectors[..., half:], vectors[..., :half]], axis=-1)

def symbol_values(constellation_labels):
    real_part = (2 * (constellation_labels % 4) - 3).astype(jnp.float32) / ROOT_TEN
    imag_part = (2 * (constellation_labels // 4) - 3).astype(jnp.float32) / ROOT_TEN
    return jnp.concatenate([real_part, imag_part], axis=-1)

def invert_small(gram):
    width = gram.shape[-1]
    entry = [[gram[..., i, j] for j in range(width)] for i in range(width)]
    lower = [[None] * width for i in range(width)]
    for j in range(width):
        pivot = entry[j][j]
        for k in range(j):
            pivot = pivot - lower[j][k] * lower[j][k]
        lower[j][j] = jnp.sqrt(pivot)
        recip = 1.0 / lower[j][j]
        for i in range(j + 1, width):
            value = entry[i][j]
            for k in range(j):
                value = value - lower[i][k] * lower[j][k]
            lower[i][j] = value * recip
    inv_lower = [[None] * width for i in range(width)]
    for i in range(width):
        inv_lower[i][i] = 1.0 / lower[i][i]
        for j in range(i):
            value = lower[i][j] * inv_lower[j][j]
            for k in range(j + 1, i):
                value = value + lower[i][k] * inv_lower[k][j]
            inv_lower[i][j] = -value * inv_lower[i][i]
    rows = []
    for i in range(width):
        cols = []
        for j in range(width):
            start = max(i, j)
            value = inv_lower[start][i] * inv_lower[start][j]
            for k in range(start + 1, width):
                value = value + inv_lower[k][i] * inv_lower[k][j]
            cols.append(value)
        rows.append(jnp.stack(cols, axis=-1))
    return jnp.stack(rows, axis=-2)

def filters_of(basis, noise):
    width = basis.shape[-2]
    eye = jnp.eye(width, dtype=jnp.float32)
    gram = jnp.einsum('sik,sjk->sij', basis, basis, precision=lax.Precision.HIGHEST) + noise[:, None, None] * eye
    inverse = invert_small(gram)
    filt = jnp.einsum('sij,sjk->sik', inverse, basis, precision=lax.Precision.HIGHEST)
    diag = jnp.diagonal(inverse, axis1=1, axis2=2)[:, :width // 2]
    amplitude_level = 1.0 - noise[:, None] * diag
    return (filt, amplitude_level)

def reference(observed_vector, propagation_matrix, noise_var, sliced_constellation, detection_sequence):
    padded = jnp.pad(propagation_matrix, ((1, 1), (0, 0), (0, 0), (0, 0)))
    smooth = 0.5 * padded[1:-1] + 0.25 * (padded[:-2] + padded[2:])
    basis_all = jnp.concatenate([smooth, rotate(smooth)], axis=2)
    constellation_labels = jnp.take(sliced_constellation.reshape(TONE_COUNT, OFDM_TIME_SLOTS, CLUSTER_COUNT, TERMINAL_COUNT), detection_sequence.astype(jnp.int32), axis=2)
    symbols = symbol_values(constellation_labels)
    current = observed_vector
    results = []
    for slot in range(CLUSTER_COUNT):
        basis = basis_all[:, slot]
        filt, amplitude_level = filters_of(basis, noise_var)
        average_amplitude = lax.optimization_barrier(jnp.sum(amplitude_level, axis=0)) / TONE_COUNT
        scale = jnp.concatenate([average_amplitude, average_amplitude])
        est = jnp.einsum('sik,stk->sti', filt, current, precision=lax.Precision.HIGHEST) / scale
        results.append(est)
        remove_decided = jnp.einsum('sti,sik->stk', symbols[:, :, slot], basis, precision=lax.Precision.HIGHEST)
        current = current - remove_decided
    return jnp.concatenate(results, axis=2)
```

```python
import functools

import jax
import jax.numpy as jnp
from jax import lax
from jax.experimental import pallas as pl
from jax.experimental.pallas import tpu as pltpu
from jax.sharding import PartitionSpec as P

ROOT_TEN = 3.1622776601683795
LANES = 128


def c_mul(a, b):
    return (a[0] * b[0] - a[1] * b[1], a[0] * b[1] + a[1] * b[0])


def c_mul_conj(a, b):
    return (a[0] * b[0] + a[1] * b[1], a[1] * b[0] - a[0] * b[1])


def c_add(a, b):
    return (a[0] + b[0], a[1] + b[1])


def c_sub(a, b):
    return (a[0] - b[0], a[1] - b[1])


def invert_hermitian(entry, width):
    low = [[None] * width for _ in range(width)]
    recip = [None] * width
    for j in range(width):
        pivot = entry[j][j][0]
        for k in range(j):
            pivot = pivot - (low[j][k][0] * low[j][k][0] + low[j][k][1] * low[j][k][1])
        recip[j] = 1.0 / jnp.sqrt(pivot)
        for i in range(j + 1, width):
            value = entry[i][j]
            for k in range(j):
                value = c_sub(value, c_mul_conj(low[i][k], low[j][k]))
            low[i][j] = (value[0] * recip[j], value[1] * recip[j])
    inv_low = [[None] * width for _ in range(width)]
    zero = jnp.zeros_like(recip[0])
    for i in range(width):
        inv_low[i][i] = (recip[i], zero)
        for j in range(i):
            value = (low[i][j][0] * recip[j], low[i][j][1] * recip[j])
            for k in range(j + 1, i):
                value = c_add(value, c_mul(low[i][k], inv_low[k][j]))
            inv_low[i][j] = (-value[0] * recip[i], -value[1] * recip[i])
    inverse = [[None] * width for _ in range(width)]
    for i in range(width):
        for j in range(i + 1):
            value = c_mul_conj(inv_low[i][j], inv_low[i][i])
            for k in range(i + 1, width):
                value = c_add(value, c_mul_conj(inv_low[k][j], inv_low[k][i]))
            inverse[i][j] = value
            if i != j:
                inverse[j][i] = (value[0], -value[1])
    return inverse


def kernel(
    dims, det_ref, y_hbm, h_hbm, noise_ref, code_ref, out_ref,
    hsend, hbuf, ybuf, stage, csend, cbuf, pscr, tscr, sre, sim, gsend, gbuf, rsend, rbuf,
    load_sem, send_h, recv_h, send_c, recv_c, send_e, recv_lo, recv_hi, send_g, recv_g, send_r, recv_r,
):
    n, nc, tones, slots, users, times = dims
    total = n * nc
    rows = slots * users
    all_users = n * rows
    positions = n * slots
    fl = tones // n
    gb = LANES // users
    fb = min(gb, fl)
    repeats = gb // fb
    chunks = fl // fb
    tp = stage.shape[0] // rows
    tiles = pscr.shape[0]
    width = tiles * LANES
    half = h_hbm.shape[-1] // 2

    s = lax.axis_index("section")
    c = lax.axis_index("sc")
    me = s * nc + c

    def at(section, sc):
        return {"section": section, "sc": sc}

    def remote(src, dst, send, recv, section, sc):
        return pltpu.make_async_remote_copy(
            src_ref=src, dst_ref=dst, send_sem=send, recv_sem=recv,
            device_id=at(section, sc), device_id_type=pl.DeviceIdType.MESH,
        )

    load_h = pltpu.make_async_copy(h_hbm, hsend, load_sem.at[0])
    load_h.start()
    load_y = pltpu.make_async_copy(
        y_hbm.at[:, pl.ds(pl.multiple_of(s * fl, 8), fl), :], ybuf, load_sem.at[1]
    )
    load_y.start()

    barrier = pltpu.get_barrier_semaphore()

    def greet(d, carry):
        other = lax.rem(me + d, total)
        pl.semaphore_signal(
            barrier, inc=1, device_id=at(lax.div(other, nc), lax.rem(other, nc)),
            device_id_type=pl.DeviceIdType.MESH,
        )
        return carry

    lax.fori_loop(1, total, greet, 0)

    def span(m):
        lo, hi = max(m * fl - 1, 0), min(m * fl + fl + 1, tones)
        return lo, hi, lo - (m * fl - 1)

    for m in range(n):
        lo, hi, off = span(m)

        @pl.when(s == m)
        def _():
            pltpu.make_async_copy(
                h_hbm.at[lo:hi], hbuf.at[m, off : off + hi - lo], load_sem.at[2]
            ).start()

    stage[...] = jnp.zeros_like(stage)
    for g in range(rows):
        stage[pl.ds(g * tp, times), :] = code_ref[:, g, :].astype(jnp.float32)
    csend[...] = stage[...].T
    cbuf[s] = csend[pl.ds(pl.multiple_of(s * fl, 8), fl), :]

    @pl.when((s == 0) & (c == 0))
    def _():
        hbuf[:, 0] = jnp.zeros_like(hbuf[:, 0])

    @pl.when((s == n - 1) & (c == nc - 1))
    def _():
        hbuf[:, fl + 1] = jnp.zeros_like(hbuf[:, 0])

    load_h.wait()
    pl.semaphore_wait(barrier, total - 1)

    def main_copy(m, src_section):
        lo, hi, off = span(m)
        return remote(
            hsend.at[lo:hi], hbuf.at[src_section, off : off + hi - lo],
            send_h.at[m], recv_h.at[src_section], m, c,
        )

    def code_copy(m, src_section):
        return remote(
            csend.at[m * fl : (m + 1) * fl], cbuf.at[src_section],
            send_c.at[m], recv_c.at[src_section], m, c,
        )

    def high_copy(src_section):
        return remote(
            hsend.at[0], hbuf.at[src_section, fl + 1], send_e.at[0], recv_hi.at[src_section],
            n - 1, lax.rem(c + nc - 1, nc),
        )

    def low_copy(src_section):
        return remote(
            hsend.at[tones - 1], hbuf.at[src_section, 0], send_e.at[1], recv_lo.at[src_section],
            0, lax.rem(c + 1, nc),
        )

    @pl.when(c > 0)
    def _():
        high_copy(s).start()

    @pl.when(c < nc - 1)
    def _():
        low_copy(s).start()

    for m in range(n):

        @pl.when(s != m)
        def _():
            main_copy(m, s).start()

    for m in range(n):

        @pl.when(s != m)
        def _():
            code_copy(m, s).start()

    load_y.wait()
    for m in range(n):
        lo, hi, off = span(m)

        @pl.when(s == m)
        def _():
            pltpu.make_async_copy(
                h_hbm.at[lo:hi], hbuf.at[m, off : off + hi - lo], load_sem.at[2]
            ).wait()
            for src in range(n):
                if src != m:
                    main_copy(m, src).wait_recv()

    @pl.when((s == n - 1) & (c < nc - 1))
    def _():
        for src in range(n):
            high_copy(src).wait_recv()

    @pl.when((s == 0) & (c > 0))
    def _():
        for src in range(n):
            low_copy(src).wait_recv()

    lane = lax.broadcasted_iota(jnp.int32, (1, LANES), 1)
    turn = jnp.where(lane < half, -1.0, 1.0).astype(jnp.float32)

    def rotate(v):
        return pltpu.roll(v, half, 1) * turn

    def products(f, carry):
        parts = []
        for src in range(n):
            parts.append(
                0.5 * hbuf[src, f + 1] + 0.25 * (hbuf[src, f] + hbuf[src, f + 2])
            )
        h = jnp.concatenate(parts, axis=0)
        yf = ybuf[:, pl.ds(f, 1), :].reshape(times, LANES)
        yf = jnp.concatenate([yf, jnp.zeros((tp - times, LANES), jnp.float32)], axis=0)
        pieces = [h, rotate(h), yf, -rotate(yf)]
        spare = width - 2 * all_users - 2 * tp
        if spare:
            pieces.append(jnp.zeros((spare, LANES), jnp.float32))
        other = jnp.concatenate(pieces, axis=0)
        prod = lax.dot_general(
            h, other, (((1,), (1,)), ((), ())),
            precision=lax.Precision.HIGHEST, preferred_element_type=jnp.float32,
        )
        for k in range(tiles):
            pscr[k, pl.ds(pl.multiple_of(f * all_users, 8), all_users), :] = prod[
                :, k * LANES : (k + 1) * LANES
            ]
        return carry

    lax.fori_loop(0, fl, products, 0, unroll=4)

    gain_total = None
    weights = []
    for ch in range(chunks):
        for p in range(positions):
            for k in range(tiles):
                blk = jnp.concatenate(
                    [
                        pscr[k, pl.ds(ch * fb * all_users + p * users + u, fb, stride=all_users), :]
                        for u in range(users)
                        for _ in range(repeats)
                    ],
                    axis=0,
                )
                tscr[ch, pl.ds(p * width + k * LANES, LANES), :] = blk.T
        offset = s * fl + ch * fb
        row = lax.div(offset, LANES)
        shift = lax.rem(LANES - lax.rem(offset, LANES), LANES)
        noise = jnp.broadcast_to(noise_ref[pl.ds(row, 1), :], (8, LANES))
        noise = jnp.where(lane < fb, pltpu.roll(noise, shift, 1), 0.0)
        base = noise
        for b in range(1, users * repeats):
            noise = noise + pltpu.roll(base, fb * b, 1)
        if positions > 8:
            noise = jnp.concatenate([noise] * (positions // 8), axis=0)
        noise = noise[:positions]
        step = width + users
        d_re = [tscr[ch, pl.ds(v, positions, stride=step), :] for v in range(users)]
        d_im = [tscr[ch, pl.ds(all_users + v, positions, stride=step), :] for v in range(users)]

        def group(x, u):
            return x if u == 0 else pltpu.roll(x, LANES - gb * u, 1)

        entry = [[None] * users for _ in range(users)]
        for i in range(users):
            for j in range(i + 1):
                entry[i][j] = (group(d_re[j], i), -group(d_im[j], i))
            entry[i][i] = (entry[i][i][0] + noise, None)
        inverse = invert_hermitian(entry, users)

        def spread(values):
            result = None
            for u in range(users):
                moved = values[u] if u == 0 else pltpu.roll(values[u], gb * u, 1)
                result = moved if u == 0 else jnp.where(lane < gb * u, result, moved)
            return result

        weight = []
        for d in range(users):
            weight.append(
                (
                    spread([inverse[u][(u - d) % users][0] for u in range(users)]),
                    spread([inverse[u][(u - d) % users][1] for u in range(users)]),
                )
            )
        weights.append(weight)
        gain = 1.0 - noise * weight[0][0]
        gain_total = gain if gain_total is None else gain_total + gain

    for sp in range(n):
        gsend[sp] = gain_total[sp * slots : (sp + 1) * slots]
    gbuf[me] = gsend[s]

    def send_gain(d, carry):
        other = lax.rem(me + d, total)
        section = lax.div(other, nc)
        remote(gsend.at[section], gbuf.at[me], send_g, recv_g, section, lax.rem(other, nc)).start()
        return carry

    lax.fori_loop(1, total, send_gain, 0)

    for m in range(n):

        @pl.when(s == m)
        def _():
            for src in range(n):
                if src != m:
                    code_copy(m, src).wait_recv()

    for ch in range(chunks):
        for src in range(n):
            blk = cbuf[src, ch * fb : (ch + 1) * fb, :]
            codes = jnp.concatenate([blk] * (users * repeats), axis=0).T
            high = jnp.floor(codes * 0.25)
            re = (2.0 * (codes - 4.0 * high) - 3.0) / ROOT_TEN
            im = (2.0 * high - 3.0) / ROOT_TEN
            for slot in range(slots):
                part = slice(slot * users * tp, (slot + 1) * users * tp)
                sre[ch, src * slots + slot] = re[part]
                sim[ch, src * slots + slot] = im[part]

    for ch in range(chunks):
        for p in range(positions):
            start = p * width
            z_re = tscr[ch, pl.ds(start + 2 * all_users, tp), :]
            z_im = tscr[ch, pl.ds(start + 2 * all_users + tp, tp), :]
            for q in range(p):
                g = det_ref[q]
                for v in range(users):
                    g_re = tscr[ch, pl.ds(start + q * users + v, 1), :]
                    g_im = tscr[ch, pl.ds(start + all_users + q * users + v, 1), :]
                    s_re = sre[ch, g, v * tp : (v + 1) * tp, :]
                    s_im = sim[ch, g, v * tp : (v + 1) * tp, :]
                    z_re = z_re - (g_re * s_re + g_im * s_im)
                    z_im = z_im - (g_re * s_im - g_im * s_re)
            x_re = None
            for d in range(users):
                w_re = weights[ch][d][0][p : p + 1]
                w_im = weights[ch][d][1][p : p + 1]
                r_re = z_re if d == 0 else pltpu.roll(z_re, gb * d, 1)
                r_im = z_im if d == 0 else pltpu.roll(z_im, gb * d, 1)
                t_re = w_re * r_re - w_im * r_im
                t_im = w_re * r_im + w_im * r_re
                x_re = t_re if d == 0 else x_re + t_re
                x_im = t_im if d == 0 else x_im + t_im
            rsend[p // slots, ch, p % slots, 0] = x_re
            rsend[p // slots, ch, p % slots, 1] = x_im

    def result_copy(m, src_section):
        return remote(
            rsend.at[m], rbuf.at[src_section], send_r.at[m], recv_r.at[src_section], m, c
        )

    for m in range(n):

        @pl.when(s != m)
        def _():
            result_copy(m, s).start()

    rbuf[s] = rsend[s]

    gain_wait = remote(gbuf.at[0 : total - 1], gbuf.at[0 : total - 1], send_g, recv_g, s, c)
    gain_wait.wait_recv()
    gain_sum = jnp.sum(gbuf[...], axis=0)
    recip = []
    for u in range(users):
        own = (lane >= gb * u) & (lane < gb * (u + 1))
        mean = jnp.sum(jnp.where(own, gain_sum, 0.0), axis=1, keepdims=True) / (tones * nc * repeats)
        recip.append(1.0 / mean)

    for m in range(n):

        @pl.when(s != m)
        def _():
            result_copy(m, m).wait_recv()

    for tile in range(tones // LANES):
        for slot in range(slots):
            for ri in range(2):
                blocks = []
                for b in range(users * repeats):
                    g = tile * users * repeats + b
                    blocks.append(rbuf[g // chunks, g % chunks, slot, ri])
                for u in range(users):
                    value = None
                    for b in range(users * repeats):
                        move = (gb * (b // repeats - u)) % LANES
                        moved = pltpu.roll(blocks[b], move, 1) if move else blocks[b]
                        value = moved if b == 0 else jnp.where(lane < fb * b, value, moved)
                    value = value * recip[u][slot : slot + 1]
                    out_ref[:, slot * 2 * users + ri * users + u, tile * LANES : (tile + 1) * LANES] = value[:times]

    @pl.when(c > 0)
    def _():
        high_copy(s).wait_send()

    @pl.when(c < nc - 1)
    def _():
        low_copy(s).wait_send()

    for m in range(n):

        @pl.when(s != m)
        def _():
            main_copy(m, s).wait_send()
            code_copy(m, s).wait_send()
            result_copy(m, s).wait_send()

    gain_wait.wait_send()


def local(observed_vector, propagation_matrix, noise_var, sliced_constellation, detection_sequence):
    n, nc = lax.axis_size("section"), lax.axis_size("sc")
    tones, slots, users, depth = propagation_matrix.shape
    times = observed_vector.shape[1]
    rows = slots * users
    all_users = n * rows
    positions = n * slots
    fl = tones // n
    chunks = max(fl // (LANES // users), 1)
    tp = -(-times // 8) * 8
    tiles = -(-(2 * all_users + 2 * tp) // LANES)
    dims = (n, nc, tones, slots, users, times)
    f32 = jnp.float32
    vmem = pl.BlockSpec(memory_space=pltpu.VMEM)
    hbm = pl.BlockSpec(memory_space=pl.ANY)
    dma = pltpu.SemaphoreType.DMA
    out = pl.pallas_call(
        functools.partial(kernel, dims),
        out_shape=jax.ShapeDtypeStruct((times, 2 * rows, tones), f32),
        in_specs=[pl.BlockSpec(memory_space=pltpu.SMEM), hbm, hbm, vmem, vmem],
        out_specs=vmem,
        scratch_shapes=[
            pltpu.VMEM((tones, rows, depth), f32),
            pltpu.VMEM((n, fl + 2, rows, depth), f32),
            pltpu.VMEM((times, fl, depth), f32),
            pltpu.VMEM((rows * tp, tones), f32),
            pltpu.VMEM((tones, rows * tp), f32),
            pltpu.VMEM((n, fl, rows * tp), f32),
            pltpu.VMEM((tiles, fl * all_users, LANES), f32),
            pltpu.VMEM((chunks, positions * tiles * LANES, LANES), f32),
            pltpu.VMEM((chunks, positions, users * tp, LANES), f32),
            pltpu.VMEM((chunks, positions, users * tp, LANES), f32),
            pltpu.VMEM((n, slots, LANES), f32),
            pltpu.VMEM((n * nc, slots, LANES), f32),
            pltpu.VMEM((n, chunks, slots, 2, tp, LANES), f32),
            pltpu.VMEM((n, chunks, slots, 2, tp, LANES), f32),
            dma((3,)),
            dma((n,)), dma((n,)),
            dma((n,)), dma((n,)),
            dma((2,)), dma((n,)), dma((n,)),
            dma, dma,
            dma((n,)), dma((n,)),
        ],
        compiler_params=pltpu.CompilerParams(collective_id=0, has_side_effects=True),
    )(
        detection_sequence,
        jnp.transpose(observed_vector, (1, 0, 2)),
        propagation_matrix.reshape(tones, rows, depth),
        noise_var.reshape(tones // LANES, LANES),
        jnp.transpose(sliced_constellation, (1, 2, 0)),
    )
    return jnp.transpose(out, (2, 0, 1))


def solution(mesh):
    in_specs = (
        P("sc", None, None),
        P("sc", "section", None, None),
        P("sc"),
        P("sc", None, "section"),
        P(),
    )
    out_specs = P("sc", None, "section")
    return jax.shard_map(local, mesh=mesh, in_specs=in_specs, out_specs=out_specs, check_vma=False)
```

```python
import functools

import jax
import jax.numpy as jnp
from jax import lax
from jax.experimental import pallas as pl
from jax.experimental.pallas import tpu as pltpu
from jax.sharding import PartitionSpec as P

ROOT_TEN = 3.1622776601683795
LANES = 128


def c_mul(a, b):
    return (a[0] * b[0] - a[1] * b[1], a[0] * b[1] + a[1] * b[0])


def c_mul_conj(a, b):
    return (a[0] * b[0] + a[1] * b[1], a[1] * b[0] - a[0] * b[1])


def c_add(a, b):
    return (a[0] + b[0], a[1] + b[1])


def c_sub(a, b):
    return (a[0] - b[0], a[1] - b[1])


def invert_hermitian(entry, width):
    low = [[None] * width for _ in range(width)]
    recip = [None] * width
    for j in range(width):
        pivot = entry[j][j][0]
        for k in range(j):
            pivot = pivot - (low[j][k][0] * low[j][k][0] + low[j][k][1] * low[j][k][1])
        recip[j] = 1.0 / jnp.sqrt(pivot)
        for i in range(j + 1, width):
            value = entry[i][j]
            for k in range(j):
                value = c_sub(value, c_mul_conj(low[i][k], low[j][k]))
            low[i][j] = (value[0] * recip[j], value[1] * recip[j])
    inv_low = [[None] * width for _ in range(width)]
    zero = jnp.zeros_like(recip[0])
    for i in range(width):
        inv_low[i][i] = (recip[i], zero)
        for j in range(i):
            value = (low[i][j][0] * recip[j], low[i][j][1] * recip[j])
            for k in range(j + 1, i):
                value = c_add(value, c_mul(low[i][k], inv_low[k][j]))
            inv_low[i][j] = (-value[0] * recip[i], -value[1] * recip[i])
    inverse = [[None] * width for _ in range(width)]
    for i in range(width):
        for j in range(i + 1):
            value = c_mul_conj(inv_low[i][j], inv_low[i][i])
            for k in range(i + 1, width):
                value = c_add(value, c_mul_conj(inv_low[k][j], inv_low[k][i]))
            inverse[i][j] = value
            if i != j:
                inverse[j][i] = (value[0], -value[1])
    return inverse


def kernel(
    dims, det_ref, y_hbm, h_hbm, noise_ref, code_ref, out_ref,
    hsend, hbuf, ybuf, stage, csend, cbuf, pscr, tscr, sre, sim, gsend, gbuf, rsend, rbuf,
    load_sem, send_h, recv_h, send_c, recv_c, send_e, recv_lo, recv_hi, send_g, recv_g, send_r, recv_r,
):
    n, nc, tones, slots, users, times = dims
    total = n * nc
    rows = slots * users
    all_users = n * rows
    positions = n * slots
    fl = tones // n
    gb = LANES // users
    fb = min(gb, fl)
    repeats = gb // fb
    chunks = fl // fb
    tp = stage.shape[0] // rows
    tiles = pscr.shape[0]
    width = tiles * LANES
    half = h_hbm.shape[-1] // 2

    s = lax.axis_index("section")
    c = lax.axis_index("sc")
    me = s * nc + c

    def at(section, sc):
        return {"section": section, "sc": sc}

    def remote(src, dst, send, recv, section, sc):
        return pltpu.make_async_remote_copy(
            src_ref=src, dst_ref=dst, send_sem=send, recv_sem=recv,
            device_id=at(section, sc), device_id_type=pl.DeviceIdType.MESH,
        )

    load_h = pltpu.make_async_copy(h_hbm, hsend, load_sem.at[0])
    load_h.start()
    load_y = pltpu.make_async_copy(
        y_hbm.at[:, pl.ds(pl.multiple_of(s * fl, 8), fl), :], ybuf, load_sem.at[1]
    )
    load_y.start()

    barrier = pltpu.get_barrier_semaphore()

    def wrap(value, size):
        return jnp.where(value >= size, value - size, value)

    def for_others(act):
        for ds in reversed(range(n)):
            section = wrap(s + ds, n)

            def body(d, carry):
                act(section, wrap(c + d, nc))
                return carry

            lax.fori_loop(0 if ds else 1, nc, body, 0, unroll=True if nc <= 8 else 4)

    def greet(section, sc):
        pl.semaphore_signal(
            barrier, inc=1, device_id=at(section, sc), device_id_type=pl.DeviceIdType.MESH
        )

    for_others(greet)

    def span(m):
        lo, hi = max(m * fl - 1, 0), min(m * fl + fl + 1, tones)
        return lo, hi, lo - (m * fl - 1)

    for m in range(n):
        lo, hi, off = span(m)

        @pl.when(s == m)
        def _():
            pltpu.make_async_copy(
                h_hbm.at[lo:hi], hbuf.at[m, off : off + hi - lo], load_sem.at[2]
            ).start()

    stage[...] = jnp.zeros_like(stage)
    for g in range(rows):
        stage[pl.ds(g * tp, times), :] = code_ref[:, g, :].astype(jnp.float32)
    csend[...] = stage[...].T
    cbuf[s] = csend[pl.ds(pl.multiple_of(s * fl, 8), fl), :]

    @pl.when((s == 0) & (c == 0))
    def _():
        hbuf[:, 0] = jnp.zeros_like(hbuf[:, 0])

    @pl.when((s == n - 1) & (c == nc - 1))
    def _():
        hbuf[:, fl + 1] = jnp.zeros_like(hbuf[:, 0])

    load_h.wait()
    pl.semaphore_wait(barrier, total - 1)

    pieces_of = send_h.shape[1]
    part = fl // pieces_of

    def main_copy(m, src_section, k):
        lo, hi, off = span(m)
        first = max(off, k * part + 2 if k else 0)
        last = min(off + hi - lo, (k + 1) * part + 2)
        start = m * fl - 1
        return remote(
            hsend.at[start + first : start + last], hbuf.at[src_section, first:last],
            send_h.at[m, k], recv_h.at[src_section, k], m, c,
        )

    def code_copy(m, src_section):
        return remote(
            csend.at[m * fl : (m + 1) * fl], cbuf.at[src_section],
            send_c.at[m], recv_c.at[src_section], m, c,
        )

    def high_copy(src_section):
        return remote(
            hsend.at[0], hbuf.at[src_section, fl + 1], send_e.at[0], recv_hi.at[src_section],
            n - 1, lax.rem(c + nc - 1, nc),
        )

    def low_copy(src_section):
        return remote(
            hsend.at[tones - 1], hbuf.at[src_section, 0], send_e.at[1], recv_lo.at[src_section],
            0, lax.rem(c + 1, nc),
        )

    @pl.when(c > 0)
    def _():
        high_copy(s).start()

    @pl.when(c < nc - 1)
    def _():
        low_copy(s).start()

    for k in range(pieces_of):
        for m in range(n):

            @pl.when(s != m)
            def _():
                main_copy(m, s, k).start()
                if k == 0:
                    code_copy(m, s).start()

    lane = lax.broadcasted_iota(jnp.int32, (1, LANES), 1)
    turn = jnp.where(lane < half, -1.0, 1.0).astype(jnp.float32)

    def rotate(v):
        return pltpu.roll(v, half, 1) * turn

    def products(f, carry):
        parts = []
        for src in range(n):
            parts.append(
                0.5 * hbuf[src, f + 1] + 0.25 * (hbuf[src, f] + hbuf[src, f + 2])
            )
        h = jnp.concatenate(parts, axis=0)
        yf = ybuf[:, pl.ds(f, 1), :].reshape(times, LANES)
        yf = jnp.concatenate([yf, jnp.zeros((tp - times, LANES), jnp.float32)], axis=0)
        pieces = [h, rotate(h), yf, -rotate(yf)]
        spare = width - 2 * all_users - 2 * tp
        if spare:
            pieces.append(jnp.zeros((spare, LANES), jnp.float32))
        other = jnp.concatenate(pieces, axis=0)
        prod = lax.dot_general(
            h, other, (((1,), (1,)), ((), ())),
            precision=lax.Precision.HIGHEST, preferred_element_type=jnp.float32,
        )
        for k in range(tiles):
            pscr[k, pl.ds(pl.multiple_of(f * all_users, 8), all_users), :] = prod[
                :, k * LANES : (k + 1) * LANES
            ]
        return carry

    def make_symbols():
        for m in range(n):

            @pl.when(s == m)
            def _():
                for src in range(n):
                    if src != m:
                        code_copy(m, src).wait_recv()

        for ch in range(chunks):
            for src in range(n):
                blk = cbuf[src, ch * fb : (ch + 1) * fb, :]
                codes = jnp.concatenate([blk] * (users * repeats), axis=0).T
                high = jnp.floor(codes * 0.25)
                re = (2.0 * (codes - 4.0 * high) - 3.0) / ROOT_TEN
                im = (2.0 * high - 3.0) / ROOT_TEN
                for slot in range(slots):
                    own = slice(slot * users * tp, (slot + 1) * users * tp)
                    sre[ch, src * slots + slot] = re[own]
                    sim[ch, src * slots + slot] = im[own]

    load_y.wait()

    @pl.when((s == 0) & (c > 0))
    def _():
        for src in range(n):
            low_copy(src).wait_recv()

    for k in range(pieces_of):
        for m in range(n):
            lo, hi, off = span(m)

            @pl.when(s == m)
            def _():
                if k == 0:
                    pltpu.make_async_copy(
                        h_hbm.at[lo:hi], hbuf.at[m, off : off + hi - lo], load_sem.at[2]
                    ).wait()
                for src in range(n):
                    if src != m:
                        main_copy(m, src, k).wait_recv()

        if k == pieces_of - 1:

            @pl.when((s == n - 1) & (c < nc - 1))
            def _():
                for src in range(n):
                    high_copy(src).wait_recv()

        lax.fori_loop(k * part, (k + 1) * part, products, 0, unroll=min(8, part))
        if k == pieces_of // 2 - 1:
            make_symbols()

    gain_total = None
    weights = []
    for ch in range(chunks):
        for p in range(positions):
            for k in range(tiles):
                blk = jnp.concatenate(
                    [
                        pscr[k, pl.ds(ch * fb * all_users + p * users + u, fb, stride=all_users), :]
                        for u in range(users)
                        for _ in range(repeats)
                    ],
                    axis=0,
                )
                tscr[ch, pl.ds(p * width + k * LANES, LANES), :] = blk.T
        offset = s * fl + ch * fb
        row = lax.div(offset, LANES)
        shift = lax.rem(LANES - lax.rem(offset, LANES), LANES)
        noise = jnp.broadcast_to(noise_ref[pl.ds(row, 1), :], (8, LANES))
        noise = jnp.where(lane < fb, pltpu.roll(noise, shift, 1), 0.0)
        base = noise
        for b in range(1, users * repeats):
            noise = noise + pltpu.roll(base, fb * b, 1)
        if positions > 8:
            noise = jnp.concatenate([noise] * (positions // 8), axis=0)
        noise = noise[:positions]
        step = width + users
        d_re = [tscr[ch, pl.ds(v, positions, stride=step), :] for v in range(users)]
        d_im = [tscr[ch, pl.ds(all_users + v, positions, stride=step), :] for v in range(users)]

        def group(x, u):
            return x if u == 0 else pltpu.roll(x, LANES - gb * u, 1)

        entry = [[None] * users for _ in range(users)]
        for i in range(users):
            for j in range(i + 1):
                entry[i][j] = (group(d_re[j], i), -group(d_im[j], i))
            entry[i][i] = (entry[i][i][0] + noise, None)
        inverse = invert_hermitian(entry, users)

        def spread(values):
            result = None
            for u in range(users):
                moved = values[u] if u == 0 else pltpu.roll(values[u], gb * u, 1)
                result = moved if u == 0 else jnp.where(lane < gb * u, result, moved)
            return result

        weight = []
        for d in range(users):
            weight.append(
                (
                    spread([inverse[u][(u - d) % users][0] for u in range(users)]),
                    spread([inverse[u][(u - d) % users][1] for u in range(users)]),
                )
            )
        weights.append(weight)
        gain = 1.0 - noise * weight[0][0]
        gain_total = gain if gain_total is None else gain_total + gain

    for sp in range(n):
        gsend[sp] = gain_total[sp * slots : (sp + 1) * slots]
    gbuf[me] = gsend[s]

    def send_gain(section, sc):
        remote(gsend.at[section], gbuf.at[me], send_g, recv_g, section, sc).start()

    for_others(send_gain)

    def result_copy(m, src_section):
        return remote(
            rsend.at[m], rbuf.at[src_section], send_r.at[m], recv_r.at[src_section], m, c
        )

    for p in range(positions):
        for ch in range(chunks):
            start = p * width
            z_re = tscr[ch, pl.ds(start + 2 * all_users, tp), :]
            z_im = tscr[ch, pl.ds(start + 2 * all_users + tp, tp), :]
            for q in range(p):
                g = det_ref[q]
                for v in range(users):
                    g_re = tscr[ch, pl.ds(start + q * users + v, 1), :]
                    g_im = tscr[ch, pl.ds(start + all_users + q * users + v, 1), :]
                    s_re = sre[ch, g, v * tp : (v + 1) * tp, :]
                    s_im = sim[ch, g, v * tp : (v + 1) * tp, :]
                    z_re = z_re - (g_re * s_re + g_im * s_im)
                    z_im = z_im - (g_re * s_im - g_im * s_re)
            x_re = None
            for d in range(users):
                w_re = weights[ch][d][0][p : p + 1]
                w_im = weights[ch][d][1][p : p + 1]
                r_re = z_re if d == 0 else pltpu.roll(z_re, gb * d, 1)
                r_im = z_im if d == 0 else pltpu.roll(z_im, gb * d, 1)
                t_re = w_re * r_re - w_im * r_im
                t_im = w_re * r_im + w_im * r_re
                x_re = t_re if d == 0 else x_re + t_re
                x_im = t_im if d == 0 else x_im + t_im
            rsend[p // slots, ch, p % slots, 0] = x_re
            rsend[p // slots, ch, p % slots, 1] = x_im
        if p % slots == slots - 1:

            @pl.when(s != p // slots)
            def _():
                result_copy(p // slots, s).start()


    rbuf[s] = rsend[s]

    gain_wait = remote(gbuf.at[0 : total - 1], gbuf.at[0 : total - 1], send_g, recv_g, s, c)
    gain_wait.wait_recv()
    gain_sum = jnp.sum(gbuf[...], axis=0)
    recip = []
    for u in range(users):
        own = (lane >= gb * u) & (lane < gb * (u + 1))
        mean = jnp.sum(jnp.where(own, gain_sum, 0.0), axis=1, keepdims=True) / (tones * nc * repeats)
        recip.append(1.0 / mean)

    for m in range(n):

        @pl.when(s != m)
        def _():
            result_copy(m, m).wait_recv()

    for tile in range(tones // LANES):
        for slot in range(slots):
            for ri in range(2):
                blocks = []
                for b in range(users * repeats):
                    g = tile * users * repeats + b
                    blocks.append(rbuf[g // chunks, g % chunks, slot, ri])
                for u in range(users):
                    value = None
                    for b in range(users * repeats):
                        move = (gb * (b // repeats - u)) % LANES
                        moved = pltpu.roll(blocks[b], move, 1) if move else blocks[b]
                        value = moved if b == 0 else jnp.where(lane < fb * b, value, moved)
                    value = value * recip[u][slot : slot + 1]
                    out_ref[:, slot * 2 * users + ri * users + u, tile * LANES : (tile + 1) * LANES] = value[:times]

    @pl.when(c > 0)
    def _():
        high_copy(s).wait_send()

    @pl.when(c < nc - 1)
    def _():
        low_copy(s).wait_send()

    for m in range(n):

        @pl.when(s != m)
        def _():
            for k in range(pieces_of):
                main_copy(m, s, k).wait_send()
            code_copy(m, s).wait_send()
            result_copy(m, s).wait_send()

    gain_wait.wait_send()


def local(observed_vector, propagation_matrix, noise_var, sliced_constellation, detection_sequence):
    n, nc = lax.axis_size("section"), lax.axis_size("sc")
    tones, slots, users, depth = propagation_matrix.shape
    times = observed_vector.shape[1]
    rows = slots * users
    all_users = n * rows
    positions = n * slots
    fl = tones // n
    chunks = max(fl // (LANES // users), 1)
    tp = -(-times // 8) * 8
    tiles = -(-(2 * all_users + 2 * tp) // LANES)
    pieces_of = 4 if fl % 16 == 0 else 1
    dims = (n, nc, tones, slots, users, times)
    f32 = jnp.float32
    vmem = pl.BlockSpec(memory_space=pltpu.VMEM)
    hbm = pl.BlockSpec(memory_space=pl.ANY)
    dma = pltpu.SemaphoreType.DMA
    out = pl.pallas_call(
        functools.partial(kernel, dims),
        out_shape=jax.ShapeDtypeStruct((times, 2 * rows, tones), f32),
        in_specs=[pl.BlockSpec(memory_space=pltpu.SMEM), hbm, hbm, vmem, vmem],
        out_specs=vmem,
        scratch_shapes=[
            pltpu.VMEM((tones, rows, depth), f32),
            pltpu.VMEM((n, fl + 2, rows, depth), f32),
            pltpu.VMEM((times, fl, depth), f32),
            pltpu.VMEM((rows * tp, tones), f32),
            pltpu.VMEM((tones, rows * tp), f32),
            pltpu.VMEM((n, fl, rows * tp), f32),
            pltpu.VMEM((tiles, fl * all_users, LANES), f32),
            pltpu.VMEM((chunks, positions * tiles * LANES, LANES), f32),
            pltpu.VMEM((chunks, positions, users * tp, LANES), f32),
            pltpu.VMEM((chunks, positions, users * tp, LANES), f32),
            pltpu.VMEM((n, slots, LANES), f32),
            pltpu.VMEM((n * nc, slots, LANES), f32),
            pltpu.VMEM((n, chunks, slots, 2, tp, LANES), f32),
            pltpu.VMEM((n, chunks, slots, 2, tp, LANES), f32),
            dma((3,)),
            dma((n, pieces_of)), dma((n, pieces_of)),
            dma((n,)), dma((n,)),
            dma((2,)), dma((n,)), dma((n,)),
            dma, dma,
            dma((n,)), dma((n,)),
        ],
        compiler_params=pltpu.CompilerParams(collective_id=0, has_side_effects=True),
    )(
        detection_sequence,
        jnp.transpose(observed_vector, (1, 0, 2)),
        propagation_matrix.reshape(tones, rows, depth),
        noise_var.reshape(tones // LANES, LANES),
        jnp.transpose(sliced_constellation, (1, 2, 0)),
    )
    return jnp.transpose(out, (2, 0, 1))


def solution(mesh):
    in_specs = (
        P("sc", None, None),
        P("sc", "section", None, None),
        P("sc"),
        P("sc", None, "section"),
        P(),
    )
    out_specs = P("sc", None, "section")
    return jax.shard_map(local, mesh=mesh, in_specs=in_specs, out_specs=out_specs, check_vma=False)
```
